32 devices in a mesh: groups: 2 (over x), cent: 16 (over z, y, core).
Axes of the slice: x: 2, y: 2, z: 4, core: 2. Of those that a mesh axis runs over, the one named last changes fastest.
Arguments:
- points: bfloat16 [1024, 768], P(('groups', 'cent')), parts along dimension 0, may hold values from -64 to 64, as said below
- centroids: bfloat16 [131072, 768], P(('groups', 'cent')), parts along dimension 0, may hold values from -1 to 1
- coarse_init: float32 [4096, 768], P(('groups', 'cent')), parts along dimension 0, may hold values from -2.4 to 2.4
- assign: int32 [131072], P(('groups', 'cent')), parts along dimension 0, may hold values from 0 to 2047, as said below
Outputs:
- level_one: bfloat16 [131072, 768], P(('groups', 'cent')), parts along dimension 0
- level_two: float32 [4096, 768], P(('groups', 'cent')), parts along dimension 0
The draws below stay inside these ranges and needn't reach their ends.
There are 2 independent parts, one for each index of `groups`. The reference program is written for one: setup_inputs(seed, part) draws one part's arguments, and reference() takes and returns one part's arrays. A program takes and returns all parts, laid end to end along the dimension named above; each array names one. Nothing has to cross between parts.
Inputs may be any that keep to these rules, and one draw needn't show every extreme that they name: `points`: entries normal (clipped at 8) or uniform within 1.7; on some draws a few rows are scaled multiples of a centroid that has a close twin, giving logits up to about 300. `assign`: among the 65536 // 16 level-1 centroids held by one index of cent, at most 512 have their level-2 centroid in any one block of 2048 // 16 consecutive level-2 centroids, and some block receives exactly 512.
All inputs are finite; a program needn't handle non-finite values.
Results may differ from the reference program's by a relative error of at most 0.0039.
Values may be sent and summed in bfloat16 or wider, within the bound.
A program may use at most 64 MiB of HBM per device.

```python
import math
import jax
import jax.numpy as jnp
from jax import lax

D = 768
K1 = 65536
K2 = 2048
PTS = 512
CAP = 512
N_CENT = 16


def pair_draw(key):
    key_pts, key_cen = jax.random.split(jax.random.fold_in(key, 7), 2)
    points = jnp.clip(jax.random.normal(key_pts, (PTS, D), jnp.float32), -8.0, 8.0)
    cents = jnp.clip(0.1 * jax.random.normal(key_cen, (K1, D), jnp.float32), -0.8, 0.8)
    return (points, cents)


def draw_points(key, part):
    return pair_draw(key)[0].astype(jnp.bfloat16)


def draw_centroids(key, part):
    return pair_draw(key)[1].astype(jnp.bfloat16)


def draw_assign(key, part):
    local = K1 // N_CENT
    own = K2 // N_CENT
    limit = CAP

    def one_block(block_key):
        key_perm, key_mix, key_inner = jax.random.split(block_key, 3)
        owners = jax.random.permutation(key_perm, N_CENT)
        dest = owners[jnp.arange(local, dtype=jnp.int32) // limit]
        dest = jax.random.permutation(key_mix, dest)
        inner = jax.random.randint(key_inner, (local,), 0, own, jnp.int32)
        return dest.astype(jnp.int32) * own + inner
    keys = jax.random.split(jax.random.fold_in(key, 11), N_CENT)
    return jax.vmap(one_block)(keys).reshape(K1).astype(jnp.int32)


def level_of(stream_key, extent, pieces, least, top_value):
    def one(axis_at, blocks):
        steps = jax.random.uniform(jax.random.fold_in(jax.random.fold_in(stream_key, 6), axis_at), (blocks,), jnp.float32, least / len(pieces), top_value / len(pieces))
        return jnp.repeat(jnp.exp(steps), extent[axis_at] // blocks).reshape((-1,) + (1,) * (len(extent) - axis_at - 1))

    gain = one(*pieces[0])
    for cut in pieces[1:]:
        gain = gain * one(*cut)
    return gain


def bell_draw(key, shape, spread, most, cuts=(), kind=jnp.bfloat16):
    drawn = jax.random.normal(key, shape, jnp.float32) * spread
    if len(cuts) > 0:
        drawn = level_of(key, shape, cuts, -0.22, 0.18) * drawn
    return jnp.clip(drawn, min=-most, max=most).astype(kind)


def setup_inputs(seed: int = 0, part: int = 0) -> dict:
    key_of = jax.random.split(jax.random.key(seed), 5)
    part_splits = jax.random.split(jax.random.fold_in(key_of[4], part), 5)
    points = draw_points(jax.random.fold_in(jax.random.fold_in(key_of[4], part), 71), part)
    centroids = draw_centroids(jax.random.fold_in(jax.random.fold_in(key_of[4], part), 71), part)
    coarse_init = bell_draw(part_splits[2], (K2, D), 0.3, 2.4, ((0, 16),), jnp.float32)
    assign = draw_assign(jax.random.fold_in(jax.random.fold_in(key_of[4], part), 71), part)
    return dict(points=points, centroids=centroids, coarse_init=coarse_init, assign=assign)


TEMP = 0.05
PRIOR_ONE = 0.02
PRIOR_TWO = 0.25

def reference(points, centroids, coarse_init, assign):
    scale = 1.0 / (TEMP * math.sqrt(D))
    width = min(4096, K1)
    cblocks = centroids.reshape(K1 // width, width, D)

    def logits_of(block):
        return jnp.dot(points, block.T, preferred_element_type=jnp.float32) * scale

    def top_step(carry, block):
        return (jnp.maximum(carry, lax.optimization_barrier(jnp.max(logits_of(block), axis=1))), None)
    peak, _ = lax.scan(top_step, jnp.full((PTS,), -jnp.inf, jnp.float32), cblocks)

    def sum_step(carry, block):
        return (carry + lax.optimization_barrier(jnp.sum(jnp.exp(logits_of(block) - peak[:, None]), axis=1)), None)
    total, _ = lax.scan(sum_step, jnp.zeros((PTS,), jnp.float32), cblocks)

    def update(block):
        resp = jnp.exp(logits_of(block) - peak[:, None]) / total[:, None]
        mass = lax.optimization_barrier(jnp.sum(resp, axis=0))
        weighted = jnp.dot(resp.astype(jnp.bfloat16).T, points, preferred_element_type=jnp.float32)
        fresh = (weighted + PRIOR_ONE * block.astype(jnp.float32)) / (mass[:, None] + PRIOR_ONE)
        return (fresh, mass)
    fresh, mass = lax.map(update, cblocks)
    fresh = fresh.reshape(K1, D)
    mass = mass.reshape(K1)
    level_one = fresh.astype(jnp.bfloat16)
    moved = (mass[:, None] * fresh).astype(jnp.bfloat16)
    wsum = jax.ops.segment_sum(moved.astype(jnp.float32), assign, K2)
    msum = jax.ops.segment_sum(mass, assign, K2)
    level_two = (wsum + PRIOR_TWO * coarse_init) / (msum[:, None] + PRIOR_TWO)
    return (level_one, level_two)
```

```python
import functools
import math

import jax
import jax.numpy as jnp
from jax import lax
from jax.experimental import pallas as pl
from jax.experimental.pallas import tpu as pltpu
from jax.sharding import PartitionSpec as P

TEMP = 0.05
PRIOR_ONE = 0.02
PRIOR_TWO = 0.25
LANES = 128
MESH = pl.DeviceIdType.MESH
ROWS_BY_ROWS = (((1,), (1,)), ((), ()))


def log2_scale(width):
    return math.log2(math.e) / (TEMP * math.sqrt(width))


def stats_kernel(n, tile, pts_ref, cen_hbm, all_ref, lse_ref, cen, mine, theirs, cen_sem, sems):
    group, me = lax.axis_index("groups"), lax.axis_index("cent")
    rows, width = pts_ref.shape
    count = all_ref.shape[0]
    tiles = cen.shape[0] // tile
    c2 = log2_scale(width)

    def fetch(t):
        part = pl.ds(t * tile, tile)
        return pltpu.make_async_copy(cen_hbm.at[part], cen.at[part], cen_sem.at[t])

    for t in range(tiles):
        fetch(t).start()

    barrier = pltpu.get_barrier_semaphore()

    @pl.loop(1, n)
    def _(off):
        peer = lax.rem(me + off, n)
        pl.semaphore_signal(barrier, inc=1, device_id=(group, peer), device_id_type=MESH)

    pl.semaphore_wait(barrier, n - 1)

    here = pl.ds(pl.multiple_of(me * rows, rows), rows)

    @pl.loop(1, n)
    def _(off):
        pltpu.make_async_remote_copy(
            src_ref=pts_ref,
            dst_ref=all_ref.at[here],
            send_sem=sems.at[0],
            recv_sem=sems.at[1],
            device_id=(group, lax.rem(me + off, n)),
            device_id_type=MESH,
        ).start()

    all_ref[here, :] = pts_ref[...]
    others = all_ref.at[pl.ds(0, (n - 1) * rows)]
    pltpu.make_async_copy(others, others, sems.at[1]).wait()

    peak = jnp.full((1, count), -jnp.inf, jnp.float32)
    total = jnp.zeros((1, count), jnp.float32)

    def step(t, carry):
        peak, total = carry
        fetch(t).wait()
        block = cen[pl.ds(pl.multiple_of(t * tile, tile), tile), :]
        logits = (
            lax.dot_general(block, all_ref[...], ROWS_BY_ROWS, preferred_element_type=jnp.float32)
            * c2
        )
        higher = jnp.maximum(peak, jnp.max(logits, axis=0, keepdims=True))
        total = total * jnp.exp2(peak - higher) + jnp.sum(
            jnp.exp2(logits - higher), axis=0, keepdims=True
        )
        return higher, total

    peak, total = lax.fori_loop(0, tiles, step, (peak, total))
    mine[0:1, :] = peak
    mine[1:2, :] = total

    @pl.loop(1, n)
    def _(off):
        pltpu.make_async_remote_copy(
            src_ref=mine,
            dst_ref=theirs.at[off - 1],
            send_sem=sems.at[2],
            recv_sem=sems.at[3],
            device_id=(group, lax.rem(me + off, n)),
            device_id_type=MESH,
        ).start()

    pltpu.make_async_copy(theirs, theirs, sems.at[3]).wait()
    both = theirs[...]
    top = jnp.maximum(peak, jnp.max(both[:, 0:1, :], axis=0))
    denom = total * jnp.exp2(peak - top) + jnp.sum(
        both[:, 1:2, :] * jnp.exp2(both[:, 0:1, :] - top[None]), axis=0
    )
    lse_ref[...] = top + jnp.log2(denom)
    pltpu.make_async_copy(others, others, sems.at[0]).wait()
    pltpu.make_async_copy(theirs, theirs, sems.at[2]).wait()


def update_kernel(cen_ref, pts_ref, lse_ref, one_ref, moved_ref, mass_ref):
    tile, width = cen_ref.shape
    cen, pts = cen_ref[...], pts_ref[...]
    logits = lax.dot_general(cen, pts, ROWS_BY_ROWS, preferred_element_type=jnp.float32)
    resp = jnp.exp2(logits * log2_scale(width) - lse_ref[...])
    mass = jnp.sum(resp, axis=1, keepdims=True)
    weighted = jnp.dot(resp.astype(jnp.bfloat16), pts, preferred_element_type=jnp.float32)
    fresh = (weighted + PRIOR_ONE * cen.astype(jnp.float32)) * (1.0 / (mass + PRIOR_ONE))
    one_ref[...] = fresh.astype(jnp.bfloat16)
    moved_ref[...] = (mass * fresh).astype(jnp.bfloat16)
    mass_ref[...] = jnp.broadcast_to(mass, (tile, LANES)).T[0:1, :]


def coarse_kernel(
    n,
    moved_hbm,
    mass_ref,
    assign_ref,
    init_ref,
    two_ref,
    moved,
    core_out,
    core_in,
    line_out,
    line_in,
    total,
    pair_out,
    pair_in,
    moved_sem,
    core_sem,
    line_sem,
    pair_sem,
):
    group, me = lax.axis_index("groups"), lax.axis_index("cent")
    own, width = init_ref.shape
    lines = n // 4
    line, pair, core = me // 4, lax.rem(me // 2, 2), lax.rem(me, 2)

    def at(z, y, c):
        return (group, z * 4 + y * 2 + c)

    load = pltpu.make_async_copy(moved_hbm, moved, moved_sem)
    load.start()
    barrier = pltpu.get_barrier_semaphore()

    def greet(who):
        pl.semaphore_signal(barrier, inc=1, device_id=who, device_id_type=MESH)

    greet(at(line, pair, 1 - core))
    greet(at(line, 1 - pair, core))

    @pl.loop(1, lines)
    def _(off):
        greet(at(lax.rem(line + off, lines), pair, core))

    pl.semaphore_wait(barrier, lines + 1)
    load.wait()

    lane = lax.broadcasted_iota(jnp.int32, (2 * own, LANES), 1)

    def partial(z, c):
        base = z * (4 * own) + c * own
        row = lax.broadcasted_iota(jnp.int32, (2 * own, 1), 0)
        row = jnp.where(row >= own, row + own, row)
        hit = (assign_ref[...] - base) == row
        weight = jnp.sum(jnp.where(hit, mass_ref[...], 0.0), axis=1, keepdims=True)
        onehot = jnp.where(hit, 1.0, 0.0).astype(jnp.bfloat16)
        return jnp.dot(onehot, moved[...], preferred_element_type=jnp.float32), weight

    def put(dst, sums, weight):
        high = weight.astype(jnp.bfloat16).astype(jnp.float32)
        low = weight - high
        at_lane = lane[: weight.shape[0]]
        tail = jnp.where(at_lane == 0, high, jnp.where(at_lane == 1, low, 0.0))
        dst[:, :width] = sums.astype(jnp.bfloat16)
        dst[:, width:] = tail.astype(jnp.bfloat16)

    def get(src):
        tail = src[:, width:].astype(jnp.float32)
        return src[:, :width].astype(jnp.float32), jnp.sum(tail, axis=1, keepdims=True)

    def core_copy(s):
        return pltpu.make_async_remote_copy(
            src_ref=core_out.at[s],
            dst_ref=core_in.at[s],
            send_sem=core_sem.at[0, s],
            recv_sem=core_sem.at[1, s],
            device_id=at(line, pair, 1 - core),
            device_id_type=MESH,
        )

    def line_copy(s):
        return pltpu.make_async_remote_copy(
            src_ref=line_out.at[s],
            dst_ref=line_in.at[s],
            send_sem=line_sem.at[0, s],
            recv_sem=line_sem.at[1, s],
            device_id=at(lax.rem(line + 1 + s, lines), pair, core),
            device_id_type=MESH,
        )

    @pl.loop(0, lines)
    def _(s):
        z = lax.rem(line + 1 + s, lines)
        put(core_out.at[s], *partial(z, 1 - core))
        core_copy(s).start()
        sums, weight = partial(z, core)
        total[:, :width] = sums
        core_copy(s).wait_recv()
        other, other_weight = get(core_in.at[s])
        sums = total[:, :width] + other
        weight = weight + other_weight

        @pl.when(s < lines - 1)
        def _():
            put(line_out.at[s], sums, weight)
            line_copy(s).start()

        @pl.when(s == lines - 1)
        def _():
            total[:, :width] = sums
            total[:, width:] = jnp.broadcast_to(weight, (2 * own, LANES))

    @pl.loop(0, lines - 1)
    def _(s):
        line_copy(s).wait_recv()
        sums, weight = get(line_in.at[s])
        total[:, :width] = total[:, :width] + sums
        total[:, width:] = total[:, width:] + weight

    def half(y):
        rows = pl.ds(pl.multiple_of(y * own, own), own)
        return total[rows, :width], total[rows, width : width + 1]

    put(pair_out, *half(1 - pair))
    swap = pltpu.make_async_remote_copy(
        src_ref=pair_out,
        dst_ref=pair_in,
        send_sem=pair_sem.at[0],
        recv_sem=pair_sem.at[1],
        device_id=at(line, 1 - pair, core),
        device_id_type=MESH,
    )
    swap.start()
    swap.wait_recv()
    sums, weight = half(pair)
    other, other_weight = get(pair_in)
    weight = weight + other_weight
    two_ref[...] = (sums + other + PRIOR_TWO * init_ref[...]) / (weight + PRIOR_TWO)

    @pl.loop(0, lines)
    def _(s):
        core_copy(s).wait_send()

    @pl.loop(0, lines - 1)
    def _(s):
        line_copy(s).wait_send()

    swap.wait_send()


def shards(n, points, centroids, coarse_init, assign):
    rows, width = points.shape
    local = centroids.shape[0]
    own = coarse_init.shape[0]
    count = n * rows
    tile = min(512, local)
    vmem = pl.BlockSpec(memory_space=pltpu.VMEM)
    anywhere = pl.BlockSpec(memory_space=pl.ANY)
    everyone, lse = pl.pallas_call(
        functools.partial(stats_kernel, n, tile),
        out_shape=(
            jax.ShapeDtypeStruct((count, width), jnp.bfloat16),
            jax.ShapeDtypeStruct((1, count), jnp.float32),
        ),
        in_specs=[vmem, anywhere],
        out_specs=(vmem, vmem),
        scratch_shapes=[
            pltpu.VMEM((local, width), jnp.bfloat16),
            pltpu.VMEM((2, count), jnp.float32),
            pltpu.VMEM((n - 1, 2, count), jnp.float32),
            pltpu.SemaphoreType.DMA((local // tile,)),
            pltpu.SemaphoreType.DMA((4,)),
        ],
        compiler_params=pltpu.CompilerParams(collective_id=0, has_side_effects=True),
        name="stats",
    )(points, centroids)
    level_one, moved, mass = pl.pallas_call(
        update_kernel,
        grid=(local // tile,),
        out_shape=(
            jax.ShapeDtypeStruct((local, width), jnp.bfloat16),
            jax.ShapeDtypeStruct((local, width), jnp.bfloat16),
            jax.ShapeDtypeStruct((1, local), jnp.float32),
        ),
        in_specs=[
            pl.BlockSpec((tile, width), lambda t: (t, 0)),
            pl.BlockSpec((count, width), lambda t: (0, 0)),
            pl.BlockSpec((1, count), lambda t: (0, 0)),
        ],
        out_specs=(
            pl.BlockSpec((tile, width), lambda t: (t, 0)),
            pl.BlockSpec((tile, width), lambda t: (t, 0)),
            pl.BlockSpec((1, tile), lambda t: (0, t)),
        ),
        name="update",
    )(centroids, everyone, lse)
    lines = n // 4
    wide = width + LANES
    level_two = pl.pallas_call(
        functools.partial(coarse_kernel, n),
        out_shape=jax.ShapeDtypeStruct((own, width), jnp.float32),
        in_specs=[anywhere, vmem, vmem, vmem],
        out_specs=vmem,
        scratch_shapes=[
            pltpu.VMEM((local, width), jnp.bfloat16),
            pltpu.VMEM((lines, 2 * own, wide), jnp.bfloat16),
            pltpu.VMEM((lines, 2 * own, wide), jnp.bfloat16),
            pltpu.VMEM((lines, 2 * own, wide), jnp.bfloat16),
            pltpu.VMEM((lines, 2 * own, wide), jnp.bfloat16),
            pltpu.VMEM((2 * own, wide), jnp.float32),
            pltpu.VMEM((own, wide), jnp.bfloat16),
            pltpu.VMEM((own, wide), jnp.bfloat16),
            pltpu.SemaphoreType.DMA,
            pltpu.SemaphoreType.DMA((2, lines)),
            pltpu.SemaphoreType.DMA((2, lines)),
            pltpu.SemaphoreType.DMA((2,)),
        ],
        compiler_params=pltpu.CompilerParams(collective_id=1, has_side_effects=True),
        name="coarse",
    )(moved, mass, assign.reshape(1, local), coarse_init)
    return (level_one, level_two)


def solution(mesh):
    return jax.shard_map(
        functools.partial(shards, mesh.shape["cent"]),
        mesh=mesh,
        in_specs=(
            P(("groups", "cent"), None),
            P(("groups", "cent"), None),
            P(("groups", "cent"), None),
            P(("groups", "cent")),
        ),
        out_specs=(P(("groups", "cent"), None), P(("groups", "cent"), None)),
        check_vma=False,
    )
```
